32 devices in a mesh: dp: 4 (over y, z), tp: 8 (over x, core).
Axes of the slice: x: 4, y: 2, z: 2, core: 2. Of those that a mesh axis runs over, the one named last changes fastest.
The devices are a block of a 4x4x8 slice.
Arguments:
- hidden: bfloat16 [32, 9, 4096], P('dp'), parts along dimension 0
- draft_ids: int32 [32, 8], P('dp'), parts along dimension 0
- norm_gain: bfloat16 [4096], replicated
- head_w: bfloat16 [4096, 128256], P(None, 'tp')
Outputs:
- output 1: float32 [32, 8], P('dp'), parts along dimension 0
- output 2: float32 [32, 9], P('dp'), parts along dimension 0
- output 3: float32 [32, 9], P('dp'), parts along dimension 0
There are 4 independent parts. The reference program is written for one: setup_inputs(seed, part) draws one part's arguments, and reference() takes and returns one part's arrays. A program takes and returns all parts, laid end to end along the dimension named above; an argument that names none is the same for every part.
All inputs are finite; a program needn't handle non-finite values.
Results may differ from the reference program's by a relative error of at most 0.001.
Values sent between devices are 32-bit elements.
A program may use at most 768 MiB of HBM per device.

```python
import jax
import jax.numpy as jnp
from jax import lax

DIM = 4096
VOCAB = 128256
BATCH = 8
DRAFTS = 8
NORM_EPS = 1e-5


def setup_inputs(seed: int = 0, part: int = 0) -> dict:
    root_key = jax.random.key(seed)
    shared_key, part_base = jax.random.split(root_key)
    part_key = jax.random.fold_in(part_base, part)
    key_x, key_d = jax.random.split(part_key)
    key_g, key_w, key_hot = jax.random.split(shared_key, 3)
    hidden = jax.random.normal(key_x, (BATCH, DRAFTS + 1, DIM), jnp.float32)
    draft_ids = jax.random.randint(key_d, (BATCH, DRAFTS), 0, VOCAB, jnp.int32)
    norm_gain = 1.0 + 0.2 * jax.random.normal(key_g, (DIM,), jnp.float32)
    hot_cols = jax.random.randint(key_hot, (VOCAB,), 0, 64, jnp.int32) == 0
    col_scale = jnp.where(hot_cols, 3.5, 2.0) * DIM ** -0.5
    head_w = jax.random.normal(key_w, (DIM, VOCAB), jnp.float32) * col_scale
    return {'hidden': hidden.astype(jnp.bfloat16), 'draft_ids': draft_ids, 'norm_gain': norm_gain.astype(jnp.bfloat16), 'head_w': head_w.astype(jnp.bfloat16)}


def rms_norm(hidden, norm_gain):
    wide_x = hidden.astype(jnp.float32)
    inv_rms = lax.rsqrt(jnp.mean(wide_x * wide_x, axis=-1, keepdims=True) + NORM_EPS)
    return (wide_x * inv_rms * norm_gain.astype(jnp.float32)).astype(jnp.bfloat16)


def reference(hidden, draft_ids, norm_gain, head_w):
    def one_sequence(seq_pair):
        seq_rows, seq_ids = seq_pair
        normed = rms_norm(seq_rows, norm_gain)
        logits = jnp.dot(normed, head_w, preferred_element_type=jnp.float32)
        row_max = jnp.max(logits, axis=-1)
        shifted = logits - row_max[:, None]
        exp_vals = jnp.exp(shifted)
        exp_sum = jnp.sum(exp_vals, axis=-1)
        weighted = jnp.sum(exp_vals * shifted, axis=-1)
        log_sum = jnp.log(exp_sum)
        log_norm = row_max + log_sum
        entropy = log_sum - weighted / exp_sum
        drafts = seq_ids.shape[0]
        picked = jnp.take_along_axis(logits[:drafts], seq_ids[:, None], axis=1)[:, 0]
        return picked - log_norm[:drafts], log_norm, entropy
    draft_logp, log_norm, entropy = lax.map(one_sequence, (hidden, draft_ids))
    return draft_logp, log_norm, entropy
```

```python
import functools

import jax
import jax.numpy as jnp
from jax import lax
from jax.experimental import pallas as pl
from jax.experimental.pallas import tpu as pltpu
from jax.sharding import PartitionSpec as P

NORM_EPS = 1e-5
BLOCK = 512
SLOTS = 11
LANES = 128
NT = (((1,), (1,)), ((), ()))
F32 = jnp.float32


def kernel(tp, hid_hbm, ids_hbm, gain_hbm, wt_hbm, logp_ref, norm_ref, ent_ref,
           hid, ids, gain, nb, ring, logits, msgs, hid_sem, ids_sem, gain_sem, ring_sem, send_sem, recv_sem):
    steps, seqs, dim = hid_hbm.shape
    drafts = ids_hbm.shape[1]
    rows = steps * seqs
    cols = wt_hbm.shape[0]
    full = cols // BLOCK
    tail = cols - full * BLOCK
    me = lax.axis_index('tp')

    copies = (pltpu.make_async_copy(hid_hbm, hid, hid_sem), pltpu.make_async_copy(gain_hbm, gain, gain_sem),
              pltpu.make_async_copy(ids_hbm, ids, ids_sem))
    for copy in copies:
        copy.start()

    def load(block, slot):
        return pltpu.make_async_copy(wt_hbm.at[pl.ds(pl.multiple_of(block * BLOCK, BLOCK), BLOCK)], ring.at[slot], ring_sem.at[slot])

    def load_tail(slot):
        return pltpu.make_async_copy(wt_hbm.at[pl.ds(full * BLOCK, tail)], ring.at[slot, pl.ds(0, tail)], ring_sem.at[slot])

    for b in range(SLOTS):
        load(b, b).start()

    barrier = pltpu.get_barrier_semaphore()
    for step in range(1, tp):
        pl.semaphore_signal(barrier, inc=1, device_id={'tp': lax.rem(me + step, tp)}, device_id_type=pl.DeviceIdType.MESH)

    for copy in copies:
        copy.wait()

    nb[...] = jnp.zeros_like(nb)
    g = jnp.concatenate([gain[j:j + 1].astype(F32) for j in range(dim // LANES)], axis=1)

    def normed(t):
        x = hid[t].astype(F32)
        inv = lax.rsqrt(jnp.mean(x * x, axis=-1, keepdims=True) + NORM_EPS)
        return x * inv * g

    for t in range(0, steps - 1, 2):
        nb[pl.ds(t * seqs, 2 * seqs), :] = jnp.concatenate([normed(t), normed(t + 1)], axis=0).astype(jnp.bfloat16)
    if steps % 2:
        last = normed(steps - 1)
        nb[pl.ds((steps - 1) * seqs, 2 * seqs), :] = jnp.concatenate([last, jnp.zeros_like(last)], axis=0).astype(jnp.bfloat16)

    lane = lax.broadcasted_iota(jnp.int32, (seqs, LANES), 1)
    sub = lax.broadcasted_iota(jnp.int32, (seqs, LANES), 0)
    spread = jnp.full((seqs, LANES), -1, jnp.int32)
    for t in range(drafts):
        spread = jnp.where(lane // seqs == t, ids[:, t:t + 1] - me * cols, spread)
    spread = jnp.sum(jnp.where(lane % seqs == sub, spread, 0), axis=0, keepdims=True)
    id_row = jnp.where(lane[:1] < drafts * seqs, spread, -1)
    id_rel = jnp.broadcast_to(id_row, (seqs, LANES)) - sub

    def stats(carry, first, count):
        m, s, w, p = carry
        z = [logits[pl.ds(8 * j, 8), :] for j in range(count // 8)]
        tree = list(z)
        while len(tree) > 1:
            tree = [jnp.maximum(tree[i], tree[i + 1]) if i + 1 < len(tree) else tree[i] for i in range(0, len(tree), 2)]
        top = jnp.maximum(m, tree[0])
        drop = m - top
        keep = jnp.exp(drop)
        w = keep * (w + s * drop)
        s = s * keep
        off = id_rel - first
        for j in range(count // 8):
            d = z[j] - top
            e = jnp.exp(d)
            s = s + e
            w = w + e * d
            p = p + jnp.where(off == 8 * j, z[j], 0.0)
        return top, s, w, p

    low = jnp.full((8, LANES), -1e30, F32)
    zero = jnp.zeros((8, LANES), F32)

    def block_step(i, carry):
        slot = lax.rem(i, SLOTS)
        load(i, slot).wait()
        logits[...] = lax.dot_general(ring[slot], nb[...], NT, preferred_element_type=F32)
        ahead = i + SLOTS

        @pl.when(ahead < full)
        def _():
            load(ahead, slot).start()

        @pl.when(ahead == full)
        def _():
            load_tail(slot).start()

        return stats(carry, i * BLOCK, BLOCK)

    m, s, w, p = lax.fori_loop(0, full, block_step, (low, zero, zero, zero))
    slot = full % SLOTS
    load_tail(slot).wait()
    logits[pl.ds(0, tail), :] = lax.dot_general(ring[slot, 0:tail], nb[...], NT, preferred_element_type=F32)
    m, s, w, p = stats((m, s, w, p), full * BLOCK, tail)

    top = jnp.max(m, axis=0, keepdims=True)
    drop = m - top
    keep = jnp.exp(drop)
    w = jnp.sum(keep * (w + s * drop), axis=0, keepdims=True)
    s = jnp.sum(keep * s, axis=0, keepdims=True)
    p = jnp.sum(p, axis=0, keepdims=True)
    own = jnp.where(sub == 0, top, jnp.where(sub == 1, s, jnp.where(sub == 2, w, jnp.where(sub == 3, p, 0.0))))
    msgs[me] = own

    pl.semaphore_wait(barrier, tp - 1)

    def send(step):
        return pltpu.make_async_remote_copy(
            src_ref=msgs.at[me], dst_ref=msgs.at[me], send_sem=send_sem.at[step], recv_sem=recv_sem.at[step],
            device_id={'tp': lax.rem(me + step, tp)}, device_id_type=pl.DeviceIdType.MESH)

    def arrival(step):
        return pltpu.make_async_remote_copy(
            src_ref=msgs.at[me], dst_ref=msgs.at[lax.rem(me + tp - step, tp)], send_sem=send_sem.at[step], recv_sem=recv_sem.at[step],
            device_id={'tp': lax.rem(me + step, tp)}, device_id_type=pl.DeviceIdType.MESH)

    for step in range(1, tp):
        send(step).start()
    for step in range(1, tp):
        arrival(step).wait_recv()
    for step in range(1, tp):
        send(step).wait_send()

    parts = [msgs[k] for k in range(tp)]
    top = parts[0][0:1]
    for part in parts[1:]:
        top = jnp.maximum(top, part[0:1])
    s = jnp.zeros((1, LANES), F32)
    w = jnp.zeros((1, LANES), F32)
    p = jnp.zeros((1, LANES), F32)
    for part in parts:
        drop = part[0:1] - top
        keep = jnp.exp(drop)
        s = s + keep * part[1:2]
        w = w + keep * (part[2:3] + part[1:2] * drop)
        p = p + part[3:4]
    log_sum = jnp.log(s)
    log_norm = top + log_sum
    entropy = log_sum - w / s
    logp = p - log_norm

    def place(row, count):
        grid = jnp.where(lane % seqs == sub, jnp.broadcast_to(row, (seqs, LANES)), 0.0)
        out = jnp.zeros((seqs, LANES), F32)
        for t in range(count):
            col = jnp.sum(jnp.where(lane // seqs == t, grid, 0.0), axis=1, keepdims=True)
            out = jnp.where(lane == t, col, out)
        return out[:, 0:count]

    logp_ref[...] = place(logp, drafts)
    norm_ref[...] = place(log_norm, steps)
    ent_ref[...] = place(entropy, steps)


def solution(mesh):
    tp = mesh.shape['tp']

    def per_device(hidden, draft_ids, norm_gain, head_w):
        seqs, steps, dim = hidden.shape
        cols = head_w.shape[1]
        drafts = draft_ids.shape[1]
        anywhere = pl.BlockSpec(memory_space=pl.ANY)
        vmem = pl.BlockSpec(memory_space=pltpu.VMEM)
        return pl.pallas_call(
            functools.partial(kernel, tp),
            in_specs=[anywhere] * 4,
            out_specs=[vmem] * 3,
            out_shape=[jax.ShapeDtypeStruct((seqs, drafts), F32), jax.ShapeDtypeStruct((seqs, steps), F32),
                       jax.ShapeDtypeStruct((seqs, steps), F32)],
            scratch_shapes=[
                pltpu.VMEM((steps, seqs, dim), jnp.bfloat16),
                pltpu.VMEM((seqs, drafts), jnp.int32),
                pltpu.VMEM((dim // LANES, LANES), jnp.bfloat16),
                pltpu.VMEM((LANES, dim), jnp.bfloat16),
                pltpu.VMEM((SLOTS, BLOCK, dim), jnp.bfloat16),
                pltpu.VMEM((BLOCK, LANES), F32),
                pltpu.VMEM((tp, 8, LANES), F32),
                pltpu.SemaphoreType.DMA, pltpu.SemaphoreType.DMA, pltpu.SemaphoreType.DMA,
                pltpu.SemaphoreType.DMA((SLOTS,)),
                pltpu.SemaphoreType.DMA((tp,)),
                pltpu.SemaphoreType.DMA((tp,)),
            ],
            compiler_params=pltpu.CompilerParams(collective_id=0, has_side_effects=True, vmem_limit_bytes=60 * 2**20),
        )(hidden.transpose(1, 0, 2), draft_ids, norm_gain.reshape(dim // LANES, LANES), head_w.T)

    specs_in = (P('dp', None, None), P('dp', None), P(None), P(None, 'tp'))
    specs_out = (P('dp', None), P('dp', None), P('dp', None))
    return jax.shard_map(per_device, mesh=mesh, in_specs=specs_in, out_specs=specs_out, check_vma=False)
```

```python
import functools

import jax
import jax.numpy as jnp
from jax import lax
from jax.experimental import pallas as pl
from jax.experimental.pallas import tpu as pltpu
from jax.sharding import PartitionSpec as P

NORM_EPS = 1e-5
BLOCK = 512
SLOTS = 4
ALONE = 12
PIECES = 4
LANES = 128
NT = (((1,), (1,)), ((), ()))
F32 = jnp.float32
MESH = pl.DeviceIdType.MESH


def kernel(tp, hid_hbm, ids_hbm, gain_hbm, wt_hbm, out_ref,
           hid, ids, far_ids, gain, near_f32, far_f32, nb, ring, logits, msgs,
           hid_sem, ids_sem, gain_sem, ring_sem, z_send, z_recv, d_send, d_recv, i_send, i_recv, send_sem, recv_sem):
    steps, seqs, dim = hid_hbm.shape
    drafts = ids_hbm.shape[1]
    rows = steps * seqs
    cols = wt_hbm.shape[0]
    alone = ALONE * BLOCK
    share = (cols - alone) // 2
    blocks = ALONE + share // BLOCK
    tail = share % BLOCK
    group, me = lax.axis_index('dp'), lax.axis_index('tp')
    side = lax.rem(group, 2)
    mate = group + 1 - 2 * side
    core = lax.rem(me, 2)
    twin = me + 1 - 2 * core

    copies = (pltpu.make_async_copy(hid_hbm, hid, hid_sem), pltpu.make_async_copy(gain_hbm, gain, gain_sem),
              pltpu.make_async_copy(ids_hbm, ids, ids_sem))
    for copy in copies:
        copy.start()

    def first_col(block):
        return pl.multiple_of(block * BLOCK + jnp.where(block >= ALONE, side * share, 0), 16)

    def load(block, slot):
        return pltpu.make_async_copy(wt_hbm.at[pl.ds(first_col(block), BLOCK)], ring.at[slot], ring_sem.at[slot])

    def load_tail(slot):
        return pltpu.make_async_copy(wt_hbm.at[pl.ds(first_col(jnp.int32(blocks)), tail)], ring.at[slot, pl.ds(0, tail)], ring_sem.at[slot])

    for b in range(SLOTS):
        load(b, b).start()

    def peers():
        for k in range(1, tp):
            yield group, lax.rem(me + k, tp)
        for k in range(tp):
            yield mate, lax.rem(me + k, tp)

    barrier = pltpu.get_barrier_semaphore()
    for g, t in peers():
        pl.semaphore_signal(barrier, inc=1, device_id={'dp': g, 'tp': t}, device_id_type=MESH)

    for copy in copies:
        copy.wait()

    scale = jnp.concatenate([gain[j:j + 1].astype(F32) for j in range(dim // LANES)], axis=1)
    for t in range(steps):
        x = hid[t].astype(F32)
        inv = lax.rsqrt(jnp.mean(x * x, axis=-1, keepdims=True) + NORM_EPS)
        near_f32[pl.ds(t * seqs, seqs), :] = (x * inv * scale).astype(jnp.bfloat16).astype(F32)

    pl.semaphore_wait(barrier, 2 * tp - 1)

    half = dim // 2
    width = half // PIECES

    def columns(c, k):
        return pl.ds(pl.multiple_of(c * half + k * width, LANES), width)

    def across(k):
        return pltpu.make_async_remote_copy(
            src_ref=near_f32.at[:, columns(core, k)], dst_ref=far_f32.at[:, columns(core, k)],
            send_sem=z_send.at[k], recv_sem=z_recv.at[k], device_id={'dp': mate, 'tp': me}, device_id_type=MESH)

    def onward(k):
        return pltpu.make_async_remote_copy(
            src_ref=far_f32.at[:, columns(core, k)], dst_ref=far_f32.at[:, columns(core, k)],
            send_sem=d_send.at[k], recv_sem=d_recv.at[k], device_id={'dp': group, 'tp': twin}, device_id_type=MESH)

    def landing(k):
        return pltpu.make_async_remote_copy(
            src_ref=far_f32.at[:, columns(core, k)], dst_ref=far_f32.at[:, columns(1 - core, k)],
            send_sem=d_send.at[k], recv_sem=d_recv.at[k], device_id={'dp': group, 'tp': twin}, device_id_type=MESH)

    ids_copy = pltpu.make_async_remote_copy(src_ref=ids, dst_ref=far_ids, send_sem=i_send, recv_sem=i_recv,
                                            device_id={'dp': mate, 'tp': me}, device_id_type=MESH)
    ids_copy.start()
    for k in range(PIECES):
        across(k).start()

    nb[...] = jnp.zeros_like(nb)
    whole = rows // 16 * 16

    def pack(base, src):
        nb[pl.ds(base, whole), :] = src[0:whole, :].astype(jnp.bfloat16)
        rest = src[whole:rows, :]
        nb[pl.ds(base + whole, 16), :] = jnp.concatenate([rest, jnp.zeros_like(rest)], axis=0).astype(jnp.bfloat16)

    pack(0, near_f32)

    lane = lax.broadcasted_iota(jnp.int32, (seqs, LANES), 1)
    sub = lax.broadcasted_iota(jnp.int32, (seqs, LANES), 0)

    def id_grid(src):
        spread = jnp.full((seqs, LANES), -1, jnp.int32)
        for t in range(drafts):
            spread = jnp.where(lane // seqs == t, src[:, t:t + 1] - me * cols, spread)
        row = jnp.sum(jnp.where(lane % seqs == sub, spread, 0), axis=0, keepdims=True)
        return jnp.broadcast_to(jnp.where(lane[:1] < drafts * seqs, row, -1), (seqs, LANES)) - sub

    def stats(carry, id_rel, buf, base, first, count):
        m, s, w, p = carry
        z = [logits[buf, pl.ds(8 * j, 8), base:base + LANES] for j in range(count // 8)]
        tree = list(z)
        while len(tree) > 1:
            tree = [jnp.maximum(tree[i], tree[i + 1]) if i + 1 < len(tree) else tree[i] for i in range(0, len(tree), 2)]
        top = jnp.maximum(m, tree[0])
        drop = m - top
        keep = jnp.exp(drop)
        w = keep * (w + s * drop)
        s = s * keep
        off = id_rel - first
        for j in range(count // 8):
            d = z[j] - top
            e = jnp.exp(d)
            s = s + e
            w = w + e * d
            p = p + jnp.where(off == 8 * j, z[j], 0.0)
        return top, s, w, p

    low = jnp.full((8, LANES), -1e30, F32)
    zero = jnp.zeros((8, LANES), F32)
    fresh = (low, zero, zero, zero)
    near_id = id_grid(ids)

    def refill(block, slot):
        @pl.when(block < blocks)
        def _():
            load(block, slot).start()

        @pl.when(block == blocks)
        def _():
            load_tail(slot).start()

    def pair(block, near, far=None, second=BLOCK):
        wide = LANES if far is None else 2 * LANES
        counts = (BLOCK, second)
        slots = [lax.rem(block + u, SLOTS) for u in range(2)]
        load(block, slots[0]).wait()
        if second == BLOCK:
            load(block + 1, slots[1]).wait()
        else:
            load_tail(slots[1]).wait()
        for u in range(2):
            logits[u, 0:counts[u], 0:wide] = lax.dot_general(ring[slots[u], 0:counts[u]], nb[0:wide], NT, preferred_element_type=F32)
        for u in range(2):
            refill(block + u + SLOTS, slots[u])
        for u in range(2):
            first = first_col(block + u)
            near = stats(near, near_id, u, 0, first, counts[u])
            if far is not None:
                far = stats(far, far_id, u, LANES, first, counts[u])
        return near, far

    near = lax.fori_loop(0, ALONE // 2, lambda i, c: pair(2 * i, c)[0], fresh)
    for k in range(PIECES):
        across(k).wait_recv()
        onward(k).start()
    ids_copy.wait_recv()
    far_id = id_grid(far_ids)
    for k in range(PIECES):
        landing(k).wait_recv()
    pack(LANES, far_f32)

    together = blocks - ALONE
    near, far = lax.fori_loop(0, together // 2, lambda i, c: pair(ALONE + 2 * i, *c), (near, fresh))
    near, far = pair(jnp.int32(blocks - 1), near, far, tail)

    def fold(carry):
        m, s, w, p = carry
        top = jnp.max(m, axis=0, keepdims=True)
        drop = m - top
        keep = jnp.exp(drop)
        w = jnp.sum(keep * (w + s * drop), axis=0, keepdims=True)
        s = jnp.sum(keep * s, axis=0, keepdims=True)
        p = jnp.sum(p, axis=0, keepdims=True)
        return jnp.where(sub == 0, top, jnp.where(sub == 1, s, jnp.where(sub == 2, w, jnp.where(sub == 3, p, 0.0))))

    own = side * tp + me
    msgs[2 * tp] = fold(far)
    msgs[own] = fold(near)

    def send(k, g, t):
        here = k < tp
        return pltpu.make_async_remote_copy(
            src_ref=msgs.at[own if here else 2 * tp], dst_ref=msgs.at[own], send_sem=send_sem.at[k], recv_sem=recv_sem.at[k],
            device_id={'dp': g, 'tp': t}, device_id_type=MESH)

    sends = []
    for k in range(1, tp):
        sends.append(send(k, group, lax.rem(me + k, tp)))
    for k in range(tp):
        sends.append(send(tp + k, mate, lax.rem(me + k, tp)))
    for copy in reversed(sends):
        copy.start()

    def arrival(k):
        source = (side if k < tp else 1 - side) * tp + lax.rem(me + 2 * tp - k, tp)
        return pltpu.make_async_remote_copy(
            src_ref=msgs.at[own], dst_ref=msgs.at[source], send_sem=send_sem.at[k], recv_sem=recv_sem.at[k],
            device_id={'dp': group, 'tp': twin}, device_id_type=MESH)

    for k in range(1, 2 * tp):
        arrival(k).wait_recv()
    out_ref[...] = msgs[0:2 * tp]
    for copy in sends:
        copy.wait_send()
    for k in range(PIECES):
        across(k).wait_send()
        onward(k).wait_send()
    ids_copy.wait_send()


def finish(parts_ref, logp_ref, norm_ref, ent_ref):
    seqs, drafts = logp_ref.shape
    steps = norm_ref.shape[1]
    lane = lax.broadcasted_iota(jnp.int32, (seqs, LANES), 1)
    sub = lax.broadcasted_iota(jnp.int32, (seqs, LANES), 0)
    parts = [parts_ref[k] for k in range(parts_ref.shape[0])]
    top = parts[0][0:1]
    for part in parts[1:]:
        top = jnp.maximum(top, part[0:1])
    s = jnp.zeros((1, LANES), F32)
    w = jnp.zeros((1, LANES), F32)
    p = jnp.zeros((1, LANES), F32)
    for part in parts:
        drop = part[0:1] - top
        keep = jnp.exp(drop)
        s = s + keep * part[1:2]
        w = w + keep * (part[2:3] + part[1:2] * drop)
        p = p + part[3:4]
    log_sum = jnp.log(s)
    log_norm = top + log_sum
    entropy = log_sum - w / s
    logp = p - log_norm

    def place(row, count):
        grid = jnp.where(lane % seqs == sub, jnp.broadcast_to(row, (seqs, LANES)), 0.0)
        out = jnp.zeros((seqs, LANES), F32)
        for t in range(count):
            col = jnp.sum(jnp.where(lane // seqs == t, grid, 0.0), axis=1, keepdims=True)
            out = jnp.where(lane == t, col, out)
        return out[:, 0:count]

    logp_ref[...] = place(logp, drafts)
    norm_ref[...] = place(log_norm, steps)
    ent_ref[...] = place(entropy, steps)


def solution(mesh):
    tp = mesh.shape['tp']

    def per_device(hidden, draft_ids, norm_gain, head_w):
        seqs, steps, dim = hidden.shape
        rows = steps * seqs
        drafts = draft_ids.shape[1]
        anywhere = pl.BlockSpec(memory_space=pl.ANY)
        vmem = pl.BlockSpec(memory_space=pltpu.VMEM)
        dma = pltpu.SemaphoreType.DMA
        parts = pl.pallas_call(
            functools.partial(kernel, tp),
            in_specs=[anywhere] * 4,
            out_specs=vmem,
            out_shape=jax.ShapeDtypeStruct((2 * tp, 8, LANES), F32),
            scratch_shapes=[
                pltpu.VMEM((steps, seqs, dim), jnp.bfloat16),
                pltpu.VMEM((seqs, drafts), jnp.int32),
                pltpu.VMEM((seqs, drafts), jnp.int32),
                pltpu.VMEM((dim // LANES, LANES), jnp.bfloat16),
                pltpu.VMEM((rows, dim), F32),
                pltpu.VMEM((rows, dim), F32),
                pltpu.VMEM((2 * LANES, dim), jnp.bfloat16),
                pltpu.VMEM((SLOTS, BLOCK, dim), jnp.bfloat16),
                pltpu.VMEM((2, BLOCK, 2 * LANES), F32),
                pltpu.VMEM((2 * tp + 1, 8, LANES), F32),
                dma, dma, dma,
                dma((SLOTS,)),
                dma((PIECES,)), dma((PIECES,)), dma((PIECES,)), dma((PIECES,)),
                dma, dma,
                dma((2 * tp,)), dma((2 * tp,)),
            ],
            compiler_params=pltpu.CompilerParams(collective_id=0, has_side_effects=True, vmem_limit_bytes=60 * 2**20),
        )(hidden.transpose(1, 0, 2), draft_ids, norm_gain.reshape(dim // LANES, LANES), head_w.T)
        return pl.pallas_call(
            finish,
            in_specs=[vmem],
            out_specs=[vmem] * 3,
            out_shape=[jax.ShapeDtypeStruct((seqs, drafts), F32), jax.ShapeDtypeStruct((seqs, steps), F32),
                       jax.ShapeDtypeStruct((seqs, steps), F32)],
        )(parts)

    specs_in = (P('dp', None, None), P('dp', None), P(None), P(None, 'tp'))
    specs_out = (P('dp', None), P('dp', None), P('dp', None))
    return jax.shard_map(per_device, mesh=mesh, in_specs=specs_in, out_specs=specs_out, check_vma=False)
```

```python
import functools

import jax
import jax.numpy as jnp
from jax import lax
from jax.experimental import pallas as pl
from jax.experimental.pallas import tpu as pltpu
from jax.sharding import PartitionSpec as P

NORM_EPS = 1e-5
BLOCK = 512
SLOTS = 12
ALONE = 8
HALVES = 2
TRIP = 4
LANES = 128
NT = (((1,), (1,)), ((), ()))
F32 = jnp.float32
MESH = pl.DeviceIdType.MESH


def kernel(tp, hid_hbm, ids_hbm, gain_hbm, wt_hbm, out_ref,
           hid, ids, far_ids, gain, near_f32, far_f32, nb, ring, logits, part, msgs,
           hid_sem, ids_sem, gain_sem, ring_sem, z_send, z_recv, d_send, d_recv, i_send, i_recv, send_sem, recv_sem):
    steps, seqs, dim = hid_hbm.shape
    drafts = ids_hbm.shape[1]
    rows = steps * seqs
    cols = wt_hbm.shape[0]
    alone = ALONE * BLOCK
    share = (cols - alone) // 2
    tail = share % BLOCK
    sharing = share // BLOCK + (tail > 0)
    last = tail or BLOCK
    depth = dim // HALVES
    lone = ALONE * HALVES
    units = lone + sharing * HALVES
    group, me = lax.axis_index('dp'), lax.axis_index('tp')
    side = lax.rem(group, 2)
    mate = group + 1 - 2 * side
    core = lax.rem(me, 2)
    twin = me + 1 - 2 * core

    copies = (pltpu.make_async_copy(hid_hbm, hid, hid_sem), pltpu.make_async_copy(gain_hbm, gain, gain_sem),
              pltpu.make_async_copy(ids_hbm, ids, ids_sem))
    for copy in copies:
        copy.start()

    def place(unit):
        own, far = unit < lone, unit - lone
        half = jnp.where(own, lax.rem(unit, HALVES), far // sharing)
        block = jnp.where(own, unit // HALVES, lax.rem(far, sharing))
        col = block * BLOCK + jnp.where(own, 0, alone + side * share)
        return pl.multiple_of(col, 16), pl.multiple_of(half * depth, LANES)

    def load(unit, slot, count=BLOCK):
        col, start = place(unit)
        return pltpu.make_async_copy(wt_hbm.at[pl.ds(col, count), pl.ds(start, depth)], ring.at[slot, pl.ds(0, count)], ring_sem.at[slot])

    def begin(unit, slot):
        far = unit - lone
        short = (far >= 0) & (lax.rem(far, sharing) == sharing - 1)

        @pl.when((unit < units) & jnp.logical_not(short))
        def _():
            load(unit, slot).start()

        @pl.when((unit < units) & short)
        def _():
            load(unit, slot, last).start()

    for u in range(TRIP):
        load(jnp.int32(u), u).start()

    def peers():
        for k in range(1, tp):
            yield group, lax.rem(me + k, tp)
        for k in range(tp):
            yield mate, lax.rem(me + k, tp)

    barrier = pltpu.get_barrier_semaphore()
    for g, t in peers():
        pl.semaphore_signal(barrier, inc=1, device_id={'dp': g, 'tp': t}, device_id_type=MESH)

    for copy in copies:
        copy.wait()

    scale = jnp.concatenate([gain[j:j + 1].astype(F32) for j in range(dim // LANES)], axis=1)
    for t in range(steps):
        x = hid[t].astype(F32)
        inv = lax.rsqrt(jnp.mean(x * x, axis=-1, keepdims=True) + NORM_EPS)
        near_f32[pl.ds(t * seqs, seqs), :] = (x * inv * scale).astype(jnp.bfloat16).astype(F32)

    for u in range(TRIP, SLOTS - TRIP):
        load(jnp.int32(u), u).start()
    pl.semaphore_wait(barrier, 2 * tp - 1)

    width = depth // 2

    def columns(c, k):
        return pl.ds(pl.multiple_of(k * depth + c * width, LANES), width)

    def across(k):
        return pltpu.make_async_remote_copy(
            src_ref=near_f32.at[:, columns(core, k)], dst_ref=far_f32.at[:, columns(core, k)],
            send_sem=z_send.at[k], recv_sem=z_recv.at[k], device_id={'dp': mate, 'tp': me}, device_id_type=MESH)

    def onward(k):
        return pltpu.make_async_remote_copy(
            src_ref=far_f32.at[:, columns(core, k)], dst_ref=far_f32.at[:, columns(core, k)],
            send_sem=d_send.at[k], recv_sem=d_recv.at[k], device_id={'dp': group, 'tp': twin}, device_id_type=MESH)

    def landing(k):
        return pltpu.make_async_remote_copy(
            src_ref=far_f32.at[:, columns(core, k)], dst_ref=far_f32.at[:, columns(1 - core, k)],
            send_sem=d_send.at[k], recv_sem=d_recv.at[k], device_id={'dp': group, 'tp': twin}, device_id_type=MESH)

    ids_copy = pltpu.make_async_remote_copy(src_ref=ids, dst_ref=far_ids, send_sem=i_send, recv_sem=i_recv,
                                            device_id={'dp': mate, 'tp': me}, device_id_type=MESH)
    ids_copy.start()
    across(0).start()

    whole = rows // 16 * 16

    def pack(base, src, start, width):
        span = pl.ds(start, width)
        nb[pl.ds(base, whole), span] = src[0:whole, span].astype(jnp.bfloat16)
        rest = src[whole:rows, span]
        nb[pl.ds(base + whole, 16), span] = jnp.concatenate([rest, jnp.zeros_like(rest)], axis=0).astype(jnp.bfloat16)
        nb[pl.ds(base + whole + 16, LANES - whole - 16), span] = jnp.zeros((LANES - whole - 16, width), jnp.bfloat16)

    pack(0, near_f32, 0, dim)

    lane = lax.broadcasted_iota(jnp.int32, (seqs, LANES), 1)
    sub = lax.broadcasted_iota(jnp.int32, (seqs, LANES), 0)

    def id_grid(src):
        spread = jnp.full((seqs, LANES), -1, jnp.int32)
        for t in range(drafts):
            spread = jnp.where(lane // seqs == t, src[:, t:t + 1] - me * cols, spread)
        row = jnp.sum(jnp.where(lane % seqs == sub, spread, 0), axis=0, keepdims=True)
        return jnp.broadcast_to(jnp.where(lane[:1] < drafts * seqs, row, -1), (seqs, LANES)) - sub

    def stats(carry, id_rel, buf, row, base, first, count):
        m, s, w, p = carry
        z = [buf[row + 8 * j:row + 8 * j + 8, base:base + LANES] for j in range(count // 8)]
        tree = list(z)
        while len(tree) > 1:
            tree = [jnp.maximum(tree[i], tree[i + 1]) if i + 1 < len(tree) else tree[i] for i in range(0, len(tree), 2)]
        top = jnp.maximum(m, tree[0])
        drop = m - top
        keep = jnp.exp(drop)
        w = keep * (w + s * drop)
        s = s * keep
        off = id_rel - first
        for j in range(count // 8):
            d = z[j] - top
            e = jnp.exp(d)
            s = s + e
            w = w + e * d
            p = p + jnp.where(off == 8 * j, z[j], 0.0)
        return top, s, w, p

    low = jnp.full((8, LANES), -1e30, F32)
    zero = jnp.zeros((8, LANES), F32)
    fresh = (low, zero, zero, zero)
    near_id = id_grid(ids)

    def product(slot, count, lanes, half):
        return lax.dot_general(ring[slot, 0:count], nb[0:lanes, half * depth:(half + 1) * depth], NT, preferred_element_type=F32)

    def arrive(unit, counts):
        slots = [lax.rem(unit + u, SLOTS) for u in range(len(counts))]
        for u, count in enumerate(counts):
            load(unit + u, slots[u], count).wait()
        for u in range(len(counts)):
            ahead = unit + u + SLOTS - TRIP
            begin(ahead, lax.rem(ahead, SLOTS))
        return slots

    def alone_trip(i, carry):
        unit = i * TRIP
        slots = arrive(unit, [BLOCK] * TRIP)
        for b in range(TRIP // HALVES):
            logits[b * BLOCK:(b + 1) * BLOCK, 0:LANES] = sum(product(slots[b * HALVES + h], BLOCK, LANES, h) for h in range(HALVES))
        for b in range(TRIP // HALVES):
            block = i * (TRIP // HALVES) + b
            carry = stats(carry, near_id, logits, b * BLOCK, 0, block * BLOCK, BLOCK)

        @pl.when(i == 1)
        def _():
            across(0).wait_send()
            across(1).start()

        @pl.when(i == 2)
        def _():
            across(0).wait_recv()
            onward(0).start()

        return carry

    near = lax.fori_loop(0, lone // TRIP, alone_trip, fresh)
    ids_copy.wait_recv()
    far_id = id_grid(far_ids)
    landing(0).wait_recv()
    pack(LANES, far_f32, 0, depth)

    def first_half(j, counts):
        unit = lone + j
        slots = arrive(unit, counts)
        for u, count in enumerate(counts):
            part[pl.ds(pl.multiple_of((j + u) * BLOCK, BLOCK), count)] = product(slots[u], count, 2 * LANES, 0)

    def second_half(j, counts, near, far):
        unit = lone + sharing + j
        slots = arrive(unit, counts)
        def settle(u, near, far):
            first = alone + side * share + (j + u) * BLOCK
            near = stats(near, near_id, logits, u * BLOCK, 0, first, counts[u])
            return near, stats(far, far_id, logits, u * BLOCK, LANES, first, counts[u])

        for u, count in enumerate(counts):
            span = pl.ds(pl.multiple_of((j + u) * BLOCK, BLOCK), count)
            logits[u * BLOCK:u * BLOCK + count] = part[span] + product(slots[u], count, 2 * LANES, 1)
            if u:
                near, far = settle(u - 1, near, far)
        return settle(len(counts) - 1, near, far)

    trips = (sharing - 1) // TRIP
    rest = [BLOCK] * (sharing - 1 - trips * TRIP) + [last]

    def first_trip(i, carry):
        first_half(i * TRIP, [BLOCK] * TRIP)

        @pl.when(i == 1)
        def _():
            across(1).wait_recv()
            onward(1).start()

        return carry

    lax.fori_loop(0, trips, first_trip, 0)
    first_half(jnp.int32(trips * TRIP), rest)
    landing(1).wait_recv()
    pack(LANES, far_f32, depth, depth)
    near, far = lax.fori_loop(0, trips, lambda i, c: second_half(i * TRIP, [BLOCK] * TRIP, *c), (near, fresh))
    near, far = second_half(jnp.int32(trips * TRIP), rest, near, far)

    def fold(carry):
        m, s, w, p = carry
        top = jnp.max(m, axis=0, keepdims=True)
        drop = m - top
        keep = jnp.exp(drop)
        w = jnp.sum(keep * (w + s * drop), axis=0, keepdims=True)
        s = jnp.sum(keep * s, axis=0, keepdims=True)
        p = jnp.sum(p, axis=0, keepdims=True)
        return jnp.where(sub == 0, top, jnp.where(sub == 1, s, jnp.where(sub == 2, w, p)))[0:4]

    own = side * tp + me
    msgs[2 * tp] = fold(far)
    msgs[own] = fold(near)

    def send(k, g, t):
        here = k < tp
        return pltpu.make_async_remote_copy(
            src_ref=msgs.at[own if here else 2 * tp], dst_ref=msgs.at[own], send_sem=send_sem.at[k], recv_sem=recv_sem.at[k],
            device_id={'dp': g, 'tp': t}, device_id_type=MESH)

    sends = []
    for k in range(1, tp):
        sends.append(send(k, group, lax.rem(me + k, tp)))
    for k in range(tp):
        sends.append(send(tp + k, mate, lax.rem(me + k, tp)))
    for copy in reversed(sends):
        copy.start()

    def arrival(k):
        source = (side if k < tp else 1 - side) * tp + lax.rem(me + 2 * tp - k, tp)
        return pltpu.make_async_remote_copy(
            src_ref=msgs.at[own], dst_ref=msgs.at[source], send_sem=send_sem.at[k], recv_sem=recv_sem.at[k],
            device_id={'dp': group, 'tp': twin}, device_id_type=MESH)

    for k in range(1, 2 * tp):
        arrival(k).wait_recv()
    out_ref[...] = msgs[0:2 * tp]
    for copy in sends:
        copy.wait_send()
    across(1).wait_send()
    for k in range(HALVES):
        onward(k).wait_send()
    ids_copy.wait_send()


def finish(parts_ref, logp_ref, norm_ref, ent_ref):
    seqs, drafts = logp_ref.shape
    steps = norm_ref.shape[1]
    lane = lax.broadcasted_iota(jnp.int32, (seqs, LANES), 1)
    sub = lax.broadcasted_iota(jnp.int32, (seqs, LANES), 0)
    parts = [parts_ref[k] for k in range(parts_ref.shape[0])]
    top = parts[0][0:1]
    for part in parts[1:]:
        top = jnp.maximum(top, part[0:1])
    s = jnp.zeros((1, LANES), F32)
    w = jnp.zeros((1, LANES), F32)
    p = jnp.zeros((1, LANES), F32)
    for part in parts:
        drop = part[0:1] - top
        keep = jnp.exp(drop)
        s = s + keep * part[1:2]
        w = w + keep * (part[2:3] + part[1:2] * drop)
        p = p + part[3:4]
    log_sum = jnp.log(s)
    log_norm = top + log_sum
    entropy = log_sum - w / s
    logp = p - log_norm

    def place(row, count):
        grid = jnp.where(lane % seqs == sub, jnp.broadcast_to(row, (seqs, LANES)), 0.0)
        out = jnp.zeros((seqs, LANES), F32)
        for t in range(count):
            col = jnp.sum(jnp.where(lane // seqs == t, grid, 0.0), axis=1, keepdims=True)
            out = jnp.where(lane == t, col, out)
        return out[:, 0:count]

    logp_ref[...] = place(logp, drafts)
    norm_ref[...] = place(log_norm, steps)
    ent_ref[...] = place(entropy, steps)


def solution(mesh):
    tp = mesh.shape['tp']

    def per_device(hidden, draft_ids, norm_gain, head_w):
        seqs, steps, dim = hidden.shape
        rows = steps * seqs
        drafts = draft_ids.shape[1]
        cols = head_w.shape[1]
        anywhere = pl.BlockSpec(memory_space=pl.ANY)
        vmem = pl.BlockSpec(memory_space=pltpu.VMEM)
        dma = pltpu.SemaphoreType.DMA
        parts = pl.pallas_call(
            functools.partial(kernel, tp),
            in_specs=[anywhere] * 4,
            out_specs=vmem,
            out_shape=jax.ShapeDtypeStruct((2 * tp, 4, LANES), F32),
            scratch_shapes=[
                pltpu.VMEM((steps, seqs, dim), jnp.bfloat16),
                pltpu.VMEM((seqs, drafts), jnp.int32),
                pltpu.VMEM((seqs, drafts), jnp.int32),
                pltpu.VMEM((dim // LANES, LANES), jnp.bfloat16),
                pltpu.VMEM((rows, dim), F32),
                pltpu.VMEM((rows, dim), F32),
                pltpu.VMEM((2 * LANES, dim), jnp.bfloat16),
                pltpu.VMEM((SLOTS, BLOCK, dim // HALVES), jnp.bfloat16),
                pltpu.VMEM((TRIP * BLOCK, 2 * LANES), F32),
                pltpu.VMEM((pl.cdiv((cols - ALONE * BLOCK) // 2, BLOCK) * BLOCK, 2 * LANES), F32),
                pltpu.VMEM((2 * tp + 1, 4, LANES), F32),
                dma, dma, dma,
                dma((SLOTS,)),
                dma((HALVES,)), dma((HALVES,)), dma((HALVES,)), dma((HALVES,)),
                dma, dma,
                dma((2 * tp,)), dma((2 * tp,)),
            ],
            compiler_params=pltpu.CompilerParams(collective_id=0, has_side_effects=True, vmem_limit_bytes=60 * 2**20),
        )(hidden.transpose(1, 0, 2), draft_ids, norm_gain.reshape(dim // LANES, LANES), head_w.T)
        return pl.pallas_call(
            finish,
            in_specs=[vmem],
            out_specs=[vmem] * 3,
            out_shape=[jax.ShapeDtypeStruct((seqs, drafts), F32), jax.ShapeDtypeStruct((seqs, steps), F32),
                       jax.ShapeDtypeStruct((seqs, steps), F32)],
        )(parts)

    specs_in = (P('dp', None, None), P('dp', None), P(None), P(None, 'tp'))
    specs_out = (P('dp', None), P('dp', None), P('dp', None))
    return jax.shard_map(per_device, mesh=mesh, in_specs=specs_in, out_specs=specs_out, check_vma=False)
```

```python
import functools

import jax
import jax.numpy as jnp
from jax import lax
from jax.experimental import pallas as pl
from jax.experimental.pallas import tpu as pltpu
from jax.sharding import PartitionSpec as P

NORM_EPS = 1e-5
BLOCK = 512
SLOTS = 24
ALONE = 4
PARTS = 4
TRIP = 8
LANES = 128
NT = (((1,), (1,)), ((), ()))
F32 = jnp.float32
MESH = pl.DeviceIdType.MESH


def kernel(tp, hid_hbm, ids_hbm, gain_hbm, wt_hbm, out_ref,
           hid, ids, far_ids, gain, near_f32, far_f32, nb, ring, logits, part, msgs,
           hid_sem, ids_sem, gain_sem, ring_sem, z_send, z_recv, d_send, d_recv, i_send, i_recv, send_sem, recv_sem):
    steps, seqs, dim = hid_hbm.shape
    drafts = ids_hbm.shape[1]
    rows = steps * seqs
    cols = wt_hbm.shape[0]
    alone = ALONE * BLOCK
    share = (cols - alone) // 2
    tail = share % BLOCK
    sharing = share // BLOCK + (tail > 0)
    last = tail or BLOCK
    depth = dim // PARTS
    lone = ALONE * PARTS
    units = lone + sharing * PARTS
    group, me = lax.axis_index('dp'), lax.axis_index('tp')
    side = lax.rem(group, 2)
    mate = group + 1 - 2 * side
    core = lax.rem(me, 2)
    twin = me + 1 - 2 * core

    copies = (pltpu.make_async_copy(hid_hbm, hid, hid_sem), pltpu.make_async_copy(gain_hbm, gain, gain_sem),
              pltpu.make_async_copy(ids_hbm, ids, ids_sem))
    for copy in copies:
        copy.start()

    def place(unit):
        own, far = unit < lone, unit - lone
        piece = jnp.where(own, lax.rem(unit, PARTS), far // sharing)
        block = jnp.where(own, unit // PARTS, lax.rem(far, sharing))
        col = block * BLOCK + jnp.where(own, 0, alone + side * share)
        return pl.multiple_of(col, 16), pl.multiple_of(piece * depth, LANES)

    def load(unit, slot, count=BLOCK):
        col, start = place(unit)
        return pltpu.make_async_copy(wt_hbm.at[pl.ds(col, count), pl.ds(start, depth)], ring.at[slot, pl.ds(0, count)], ring_sem.at[slot])

    def begin(unit, slot):
        far = unit - lone
        short = (far >= 0) & (lax.rem(far, sharing) == sharing - 1)

        @pl.when((unit < units) & jnp.logical_not(short))
        def _():
            load(unit, slot).start()

        @pl.when((unit < units) & short)
        def _():
            load(unit, slot, last).start()

    for u in range(TRIP):
        load(jnp.int32(u), u).start()

    def peers():
        for k in range(1, tp):
            yield group, lax.rem(me + k, tp)
        for k in range(tp):
            yield mate, lax.rem(me + k, tp)

    barrier = pltpu.get_barrier_semaphore()
    for g, t in peers():
        pl.semaphore_signal(barrier, inc=1, device_id={'dp': g, 'tp': t}, device_id_type=MESH)

    for copy in copies:
        copy.wait()

    scale = jnp.concatenate([gain[j:j + 1].astype(F32) for j in range(dim // LANES)], axis=1)
    for t in range(steps):
        x = hid[t].astype(F32)
        inv = lax.rsqrt(jnp.mean(x * x, axis=-1, keepdims=True) + NORM_EPS)
        near_f32[pl.ds(t * seqs, seqs), :] = (x * inv * scale).astype(jnp.bfloat16).astype(F32)

    for u in range(TRIP, SLOTS - TRIP):
        load(jnp.int32(u), u).start()
    pl.semaphore_wait(barrier, 2 * tp - 1)

    width = depth // 2

    def columns(c, k):
        return pl.ds(pl.multiple_of(k * depth + c * width, LANES), width)

    def across(k):
        return pltpu.make_async_remote_copy(
            src_ref=near_f32.at[:, columns(core, k)], dst_ref=far_f32.at[:, columns(core, k)],
            send_sem=z_send.at[k], recv_sem=z_recv.at[k], device_id={'dp': mate, 'tp': me}, device_id_type=MESH)

    def onward(k):
        return pltpu.make_async_remote_copy(
            src_ref=far_f32.at[:, columns(core, k)], dst_ref=far_f32.at[:, columns(core, k)],
            send_sem=d_send.at[k], recv_sem=d_recv.at[k], device_id={'dp': group, 'tp': twin}, device_id_type=MESH)

    def landing(k):
        return pltpu.make_async_remote_copy(
            src_ref=far_f32.at[:, columns(core, k)], dst_ref=far_f32.at[:, columns(1 - core, k)],
            send_sem=d_send.at[k], recv_sem=d_recv.at[k], device_id={'dp': group, 'tp': twin}, device_id_type=MESH)

    ids_copy = pltpu.make_async_remote_copy(src_ref=ids, dst_ref=far_ids, send_sem=i_send, recv_sem=i_recv,
                                            device_id={'dp': mate, 'tp': me}, device_id_type=MESH)
    ids_copy.start()
    across(0).start()
    whole = rows // 16 * 16

    def pack(base, src, start, width):
        span = pl.ds(start, width)
        nb[pl.ds(base, whole), span] = src[0:whole, span].astype(jnp.bfloat16)
        rest = src[whole:rows, span]
        nb[pl.ds(base + whole, 16), span] = jnp.concatenate([rest, jnp.zeros_like(rest)], axis=0).astype(jnp.bfloat16)
        nb[pl.ds(base + whole + 16, LANES - whole - 16), span] = jnp.zeros((LANES - whole - 16, width), jnp.bfloat16)

    pack(0, near_f32, 0, dim)

    lane = lax.broadcasted_iota(jnp.int32, (seqs, LANES), 1)
    sub = lax.broadcasted_iota(jnp.int32, (seqs, LANES), 0)

    def id_grid(src):
        spread = jnp.full((seqs, LANES), -1, jnp.int32)
        for t in range(drafts):
            spread = jnp.where(lane // seqs == t, src[:, t:t + 1] - me * cols, spread)
        row = jnp.sum(jnp.where(lane % seqs == sub, spread, 0), axis=0, keepdims=True)
        return jnp.broadcast_to(jnp.where(lane[:1] < drafts * seqs, row, -1), (seqs, LANES)) - sub

    def stats(carry, id_rel, buf, row, base, first, count):
        m, s, w, p = carry
        z = [buf[row + 8 * j:row + 8 * j + 8, base:base + LANES] for j in range(count // 8)]
        tree = list(z)
        while len(tree) > 1:
            tree = [jnp.maximum(tree[i], tree[i + 1]) if i + 1 < len(tree) else tree[i] for i in range(0, len(tree), 2)]
        top = jnp.maximum(m, tree[0])
        drop = m - top
        keep = jnp.exp(drop)
        w = keep * (w + s * drop)
        s = s * keep
        off = id_rel - first
        for j in range(count // 8):
            d = z[j] - top
            e = jnp.exp(d)
            s = s + e
            w = w + e * d
            p = p + jnp.where(off == 8 * j, z[j], 0.0)
        return top, s, w, p

    low = jnp.full((8, LANES), -1e30, F32)
    zero = jnp.zeros((8, LANES), F32)
    fresh = (low, zero, zero, zero)
    near_id = id_grid(ids)

    def product(slot, count, lanes, piece):
        span = pl.ds(piece * depth if isinstance(piece, int) else pl.multiple_of(piece * depth, LANES), depth)
        return lax.dot_general(ring[slot, 0:count], nb[0:lanes, span], NT, preferred_element_type=F32)

    def arrive(unit, counts):
        slots = [lax.rem(unit + u, SLOTS) for u in range(len(counts))]
        for u, count in enumerate(counts):
            load(unit + u, slots[u], count).wait()
        for u in range(len(counts)):
            ahead = unit + u + SLOTS - TRIP
            begin(ahead, lax.rem(ahead, SLOTS))
        return slots

    def alone_trip(i, carry):
        unit = i * TRIP
        slots = arrive(unit, [BLOCK] * TRIP)
        for b in range(TRIP // PARTS):
            logits[b * BLOCK:(b + 1) * BLOCK, 0:LANES] = sum(product(slots[b * PARTS + h], BLOCK, LANES, h) for h in range(PARTS))
        for b in range(TRIP // PARTS):
            block = i * (TRIP // PARTS) + b
            carry = stats(carry, near_id, logits, b * BLOCK, 0, block * BLOCK, BLOCK)

        across(i + 1).start()
        return carry

    near = lax.fori_loop(0, lone // TRIP, alone_trip, fresh)
    across(0).wait_recv()
    onward(0).start()
    part[...] = jnp.zeros_like(part)
    ids_copy.wait_recv()
    far_id = id_grid(far_ids)
    landing(0).wait_recv()
    pack(LANES, far_f32, 0, depth)

    sizes = [BLOCK] * (sharing - 1) + [last]
    middle = (sharing + 1) // 2
    runs = ((0, sizes[:middle]), (middle, sizes[middle:]))

    def gather(p, run):
        j, counts = run
        slots = arrive(lone + p * sharing + j, counts)
        for u, count in enumerate(counts):
            span = pl.ds((j + u) * BLOCK, count)
            part[span] = part[span] + product(slots[u], count, 2 * LANES, p)

    def phase(p, carry):
        gather(p, runs[0])
        across(p + 1).wait_recv()
        onward(p + 1).start()

        @pl.when(p + ALONE * PARTS // TRIP + 1 < PARTS)
        def _():
            across(p + ALONE * PARTS // TRIP + 1).start()

        gather(p, runs[1])
        landing(p + 1).wait_recv()
        pack(LANES, far_f32, pl.multiple_of((p + 1) * depth, LANES), depth)
        return carry

    lax.fori_loop(0, PARTS - 1, phase, 0)

    def conclude(run, near, far):
        j, counts = run
        slots = arrive(jnp.int32(lone + (PARTS - 1) * sharing + j), counts)

        def settle(u, near, far):
            first = alone + side * share + (j + u) * BLOCK
            near = stats(near, near_id, logits, u * BLOCK, 0, first, counts[u])
            return near, stats(far, far_id, logits, u * BLOCK, LANES, first, counts[u])

        for u, count in enumerate(counts):
            span = pl.ds((j + u) * BLOCK, count)
            logits[u * BLOCK:u * BLOCK + count] = part[span] + product(slots[u], count, 2 * LANES, PARTS - 1)
            if u:
                near, far = settle(u - 1, near, far)
        return settle(len(counts) - 1, near, far)

    near, far = near, fresh
    for run in runs:
        near, far = conclude(run, near, far)

    def fold(carry):
        m, s, w, p = carry
        top = jnp.max(m, axis=0, keepdims=True)
        drop = m - top
        keep = jnp.exp(drop)
        w = jnp.sum(keep * (w + s * drop), axis=0, keepdims=True)
        s = jnp.sum(keep * s, axis=0, keepdims=True)
        p = jnp.sum(p, axis=0, keepdims=True)
        return jnp.where(sub == 0, top, jnp.where(sub == 1, s, jnp.where(sub == 2, w, p)))[0:4]

    own = side * tp + me
    msgs[2 * tp] = fold(far)
    msgs[own] = fold(near)

    def send(k, g, t):
        here = k < tp
        return pltpu.make_async_remote_copy(
            src_ref=msgs.at[own if here else 2 * tp], dst_ref=msgs.at[own], send_sem=send_sem.at[k], recv_sem=recv_sem.at[k],
            device_id={'dp': g, 'tp': t}, device_id_type=MESH)

    sends = []
    for k in range(1, tp):
        sends.append(send(k, group, lax.rem(me + k, tp)))
    for k in range(tp):
        sends.append(send(tp + k, mate, lax.rem(me + k, tp)))
    for copy in reversed(sends):
        copy.start()

    def arrival(k):
        source = (side if k < tp else 1 - side) * tp + lax.rem(me + 2 * tp - k, tp)
        return pltpu.make_async_remote_copy(
            src_ref=msgs.at[own], dst_ref=msgs.at[source], send_sem=send_sem.at[k], recv_sem=recv_sem.at[k],
            device_id={'dp': group, 'tp': twin}, device_id_type=MESH)

    for k in range(1, 2 * tp):
        arrival(k).wait_recv()
    out_ref[...] = msgs[0:2 * tp]
    for copy in sends:
        copy.wait_send()
    for k in range(PARTS):
        across(k).wait_send()
        onward(k).wait_send()
    ids_copy.wait_send()


def finish(parts_ref, logp_ref, norm_ref, ent_ref):
    seqs, drafts = logp_ref.shape
    steps = norm_ref.shape[1]
    lane = lax.broadcasted_iota(jnp.int32, (seqs, LANES), 1)
    sub = lax.broadcasted_iota(jnp.int32, (seqs, LANES), 0)
    parts = [parts_ref[k] for k in range(parts_ref.shape[0])]
    top = parts[0][0:1]
    for part in parts[1:]:
        top = jnp.maximum(top, part[0:1])
    s = jnp.zeros((1, LANES), F32)
    w = jnp.zeros((1, LANES), F32)
    p = jnp.zeros((1, LANES), F32)
    for part in parts:
        drop = part[0:1] - top
        keep = jnp.exp(drop)
        s = s + keep * part[1:2]
        w = w + keep * (part[2:3] + part[1:2] * drop)
        p = p + part[3:4]
    log_sum = jnp.log(s)
    log_norm = top + log_sum
    entropy = log_sum - w / s
    logp = p - log_norm

    def place(row, count):
        grid = jnp.where(lane % seqs == sub, jnp.broadcast_to(row, (seqs, LANES)), 0.0)
        out = jnp.zeros((seqs, LANES), F32)
        for t in range(count):
            col = jnp.sum(jnp.where(lane // seqs == t, grid, 0.0), axis=1, keepdims=True)
            out = jnp.where(lane == t, col, out)
        return out[:, 0:count]

    logp_ref[...] = place(logp, drafts)
    norm_ref[...] = place(log_norm, steps)
    ent_ref[...] = place(entropy, steps)


def solution(mesh):
    tp = mesh.shape['tp']

    def per_device(hidden, draft_ids, norm_gain, head_w):
        seqs, steps, dim = hidden.shape
        rows = steps * seqs
        drafts = draft_ids.shape[1]
        cols = head_w.shape[1]
        anywhere = pl.BlockSpec(memory_space=pltpu.HBM)
        vmem = pl.BlockSpec(memory_space=pltpu.VMEM)
        dma = pltpu.SemaphoreType.DMA
        parts = pl.pallas_call(
            functools.partial(kernel, tp),
            in_specs=[anywhere] * 4,
            out_specs=vmem,
            out_shape=jax.ShapeDtypeStruct((2 * tp, 4, LANES), F32),
            scratch_shapes=[
                pltpu.VMEM((steps, seqs, dim), jnp.bfloat16),
                pltpu.VMEM((seqs, drafts), jnp.int32),
                pltpu.VMEM((seqs, drafts), jnp.int32),
                pltpu.VMEM((dim // LANES, LANES), jnp.bfloat16),
                pltpu.VMEM((rows, dim), F32),
                pltpu.VMEM((rows, dim), F32),
                pltpu.VMEM((2 * LANES, dim), jnp.bfloat16),
                pltpu.VMEM((SLOTS, BLOCK, dim // PARTS), jnp.bfloat16),
                pltpu.VMEM((TRIP * BLOCK, 2 * LANES), F32),
                pltpu.VMEM((pl.cdiv((cols - ALONE * BLOCK) // 2, BLOCK) * BLOCK, 2 * LANES), F32),
                pltpu.VMEM((2 * tp + 1, 4, LANES), F32),
                dma, dma, dma,
                dma((SLOTS,)),
                dma((PARTS,)), dma((PARTS,)), dma((PARTS,)), dma((PARTS,)),
                dma, dma,
                dma((2 * tp,)), dma((2 * tp,)),
            ],
            compiler_params=pltpu.CompilerParams(collective_id=0, has_side_effects=True, vmem_limit_bytes=46 * 2**20),
        )(*(pltpu.with_memory_space_constraint(x, pltpu.HBM) for x in (
            hidden.transpose(1, 0, 2), draft_ids, norm_gain.reshape(dim // LANES, LANES), head_w.T)))
        return pl.pallas_call(
            finish,
            in_specs=[vmem],
            out_specs=[vmem] * 3,
            out_shape=[jax.ShapeDtypeStruct((seqs, drafts), F32), jax.ShapeDtypeStruct((seqs, steps), F32),
                       jax.ShapeDtypeStruct((seqs, steps), F32)],
            compiler_params=pltpu.CompilerParams(vmem_limit_bytes=4 * 2**20),
        )(parts)

    specs_in = (P('dp', None, None), P('dp', None), P(None), P(None, 'tp'))
    specs_out = (P('dp', None), P('dp', None), P('dp', None))
    return jax.shard_map(per_device, mesh=mesh, in_specs=specs_in, out_specs=specs_out, check_vma=False)
```
